32 devices in a mesh: exp: 8 (over z, core), pix: 4 (over y, x).
Axes of the slice: x: 2, y: 2, z: 4, core: 2. Of those that a mesh axis runs over, the one named last changes fastest.
Arguments:
- transmission: bfloat16 [4096, 6144], P('exp', 'pix'), may hold values from 0.29882812 to 1
- inverse_var: bfloat16 [4096, 6144], P('exp', 'pix'), may hold values from 0.25 to 4
- pixel_mask: int32 [4096, 48], P('exp', 'pix'), may hold values 0 or 1
- coef: bfloat16 [4096, 256], P('exp'), may hold values from -6 to 6
- basis: bfloat16 [256, 6144], P(None, 'pix'), may hold values from -6 to 6
- coef_tangent: bfloat16 [4096, 256], P('exp', 'pix'), may hold values from -0.375 to 0.375
- basis_tangent: bfloat16 [256, 6144], P('exp', 'pix'), may hold values from -0.375 to 0.375
Outputs:
- coef_grad: float32 [4096, 256], P('exp', 'pix')
- basis_grad: float32 [256, 6144], P('exp', 'pix')
The draws below stay inside these ranges and needn't reach their ends.
All inputs are finite; a program needn't handle non-finite values. No bound on the sum of `pixel_mask` on one device may be relied on, other than what follows from the above.
Results may differ from the reference program's by a relative error of at most 0.0008.
Values may be sent and summed in bfloat16 or wider, within the bound.
A program may use at most 64 MiB of HBM per device.

```python
import math
import jax
import jax.numpy as jnp
from jax import lax

R = 256
TILE = 128
ED = 512
NE = 4096
NP = 6144


def plant(array, rng, low, high):
    extent = array.shape
    index_at = [jax.random.randint(jax.random.fold_in(rng, axis), (), 0, extent[axis]) for axis in range(len(extent))]
    array = array.at[tuple(index_at)].set(low)
    longest = extent.index(max(extent))
    index_at[longest] = (index_at[longest] + 1) % extent[longest]
    return array.at[tuple(index_at)].set(high)


def strengthened(entries, rng, source, target, shards_of, factor):
    owner, partner = [(jnp.arange(entries.shape[dim]) // (entries.shape[dim] // shards_of)).reshape([-1 if axis == dim else 1 for axis in range(entries.ndim)]) for dim in (source, target)]
    chosen = jax.random.permutation(rng, shards_of)[partner]
    strong = (owner == chosen) | (owner == (partner + shards_of // 2) % shards_of)
    return jnp.where(strong, factor * entries, entries)


def levels(key, dims, split, low, largest):
    loudness = 1.0
    for dim, blocks in split:
        draws = jax.random.uniform(jax.random.fold_in(jax.random.fold_in(key, 6), dim), (blocks,), jnp.float32, low / len(split), largest / len(split))
        loudness = loudness * jnp.repeat(jnp.exp(draws), dims[dim] // blocks).reshape((-1,) + (1,) * (len(dims) - 1 - dim))
    return loudness


def normal_values(own_key, dims, width, limit, cuts=(), dtype=jnp.bfloat16):
    result = jax.random.normal(own_key, dims, jnp.float32) * width
    if len(cuts) > 0:
        result = levels(own_key, dims, cuts, -0.22, 0.18) * result
    return jnp.clip(result, min=-limit, max=limit).astype(dtype)


def bell_draw_with(own_key, shape, width, limit, pieces, heavy, kind=jnp.bfloat16):
    entries = width * jax.random.normal(own_key, shape, jnp.float32)
    if pieces:
        entries = entries * levels(own_key, shape, pieces, -0.22, 0.18)
    return jnp.clip(strengthened(entries, jax.random.fold_in(own_key, 3), *heavy), -limit, limit).astype(kind)


def setup_inputs(seed: int = 0) -> dict:
    streams_of = jax.random.split(jax.random.key(seed), 8)
    transmission = jnp.clip(0.29882812 + 0.7011719 * jax.random.uniform(streams_of[0], (NE, NP), jnp.float32) ** levels(streams_of[0], (NE, NP), ((0, 8), (1, 4)), -0.2, 0.2), 0.29882812, 1.0).astype(jnp.bfloat16)
    inverse_var = jnp.clip(jnp.exp(math.log(4.0) - 2.7725887 * jax.random.uniform(streams_of[1], (NE, NP), jnp.float32) ** levels(streams_of[1], (NE, NP), ((0, 8), (1, 4)), -0.2, 0.2)), 0.25, 4.0).astype(jnp.bfloat16)
    pixel_mask = plant((jax.random.randint(streams_of[2], (NE, NP // TILE), 0, 4) < 3).astype(jnp.int32), jax.random.fold_in(streams_of[2], 1), 0, 1)
    coef = bell_draw_with(streams_of[3], (NE, R), 1.0, 6.0, ((0, 8),), (0, 1, 8, 2.0))
    basis = bell_draw_with(streams_of[4], (R, NP), 1.0, 6.0, ((1, 4),), (1, 0, 4, 2.0))
    coef_tangent = normal_values(streams_of[5], (NE, R), R ** -0.5, 0.375, ((0, 8), (1, 4)))
    basis_tangent = normal_values(streams_of[6], (R, NP), R ** -0.5, 0.375, ((0, 8), (1, 4)))
    return dict(transmission=transmission, inverse_var=inverse_var, pixel_mask=pixel_mask, coef=coef, basis=basis, coef_tangent=coef_tangent, basis_tangent=basis_tangent)


def reference(transmission, inverse_var, pixel_mask, coef, basis, coef_tangent, basis_tangent):
    blocks = NE // ED
    trans_b = transmission.reshape(blocks, ED, NP)
    ivar_b = inverse_var.reshape(blocks, ED, NP)
    mask_b = pixel_mask.reshape(blocks, ED, NP // TILE)
    coef_b = coef.reshape(blocks, ED, R)
    tang_b = coef_tangent.reshape(blocks, ED, R)

    def one_block(total, items):
        trans, ivar, mask, cf, tg = items
        spread = jnp.broadcast_to(mask.astype(jnp.float32)[:, :, None], (ED, NP // TILE, TILE)).reshape(ED, NP)
        tr = trans.astype(jnp.float32)
        weights = tr * tr * ivar.astype(jnp.float32) * spread
        moved = jnp.dot(tg, basis, preferred_element_type=jnp.float32) + jnp.dot(cf, basis_tangent, preferred_element_type=jnp.float32)
        weighted = (weights * moved).astype(jnp.bfloat16)
        cgrad = jnp.dot(weighted, basis.T, preferred_element_type=jnp.float32) / math.sqrt(NP)
        total = total + jnp.dot(cf.T, weighted, preferred_element_type=jnp.float32)
        return (total, cgrad)
    start = jnp.zeros((R, NP), jnp.float32)
    total, cgrads = lax.scan(one_block, start, (trans_b, ivar_b, mask_b, coef_b, tang_b))
    return (cgrads.reshape(NE, R), total / math.sqrt(NE))
```

```python
import functools
import math

import jax
import jax.numpy as jnp
from jax import lax
from jax.experimental import pallas as pl
from jax.experimental.pallas import tpu as pltpu
from jax.sharding import PartitionSpec as P

TILE = 128
WIRE = jnp.int16
TOP = 32767.0
TINY = 1e-30
MESH = pl.DeviceIdType.MESH


def split_columns(cols):
    for pieces in (3, 2):
        if cols % (pieces * TILE) == 0:
            return pieces
    return 1


def scaled(x):
    peak = jnp.maximum(jnp.max(jnp.abs(x), axis=0, keepdims=True), TINY)
    return jnp.round(x * (TOP / peak)).astype(jnp.int32).astype(WIRE), peak * (1.0 / TOP)


def restored(value, factor):
    return value.astype(jnp.int32).astype(jnp.float32) * factor


def kernel(
    n_e, n_p, pieces,
    trans_h, ivar_h, mask_h, coef_h, basis_h, ctan_h, btan_h,
    cout, bout,
    trans, ivar, mask, coef, basis, tg, fb,
    used_rows, used_cols, tang, coef_t, weights, moved, wt,
    part, swap, rs_out, rs_in, rs_fac_out, rs_fac_in,
    cpart, cs_out, cs_in, cs_fac_out, cs_fac_in,
    load_sem, own_sem,
    tg_send, tg_recv, ag_send, ag_recv, near_send, near_recv, fw_send, fw_recv,
    swap_send, swap_recv, rs_send, rs_recv, rsf_send, rsf_recv,
    cs_send, cs_recv, csf_send, csf_recv,
):
    rows, cols = trans.shape
    rank = coef.shape[1]
    width = cols // pieces
    chips = n_e // 2
    cb = rank // n_p
    order = sorted(range(1, chips), key=lambda d: abs(2 * d - chips))
    me_e, me_p = lax.axis_index("exp"), lax.axis_index("pix")
    core, chip = lax.rem(me_e, 2), me_e // 2
    partner = chip * 2 + (1 - core)

    def over(d):
        return lax.rem(chip + d, chips)

    def back(d):
        return lax.rem(chip + chips - d, chips)

    def remote(src, dst, send, recv, e, p):
        return pltpu.make_async_remote_copy(
            src_ref=src, dst_ref=dst, send_sem=send, recv_sem=recv,
            device_id=(e, p), device_id_type=MESH,
        )

    own = []
    for j in range(pieces):
        own.append(pltpu.make_async_copy(
            btan_h.at[:, pl.ds(j * width, width)], fb.at[j, me_e], own_sem.at[j]))
    own.append(pltpu.make_async_copy(ctan_h, tg.at[me_p], own_sem.at[pieces]))
    for copy in own:
        copy.start()
    loads = [
        pltpu.make_async_copy(src, dst, load_sem.at[i])
        for i, (src, dst) in enumerate((
            (trans_h, trans), (ivar_h, ivar), (mask_h, mask), (coef_h, coef), (basis_h, basis)))
    ]
    for copy in loads:
        copy.start()

    barrier = pltpu.get_barrier_semaphore()
    for d in range(1, chips):
        pl.semaphore_signal(barrier, inc=1, device_id=(over(d) * 2 + core, me_p), device_id_type=MESH)
    pl.semaphore_signal(barrier, inc=1, device_id=(partner, me_p), device_id_type=MESH)
    for d in range(1, n_p):
        pl.semaphore_signal(barrier, inc=1, device_id=(me_e, lax.rem(me_p + d, n_p)), device_id_type=MESH)
    pl.semaphore_wait(barrier, chips + n_p - 1)

    sends = []

    def go(copy):
        copy.start()
        sends.append(copy)
        return copy

    gather, near = {}, {}
    for j in range(pieces):
        own[j].wait()
        for d in order:
            gather[j, d] = go(remote(fb.at[j, me_e], fb.at[j, me_e], ag_send.at[j, d], ag_recv.at[j, d],
                                     over(d) * 2 + core, me_p))
        near[j] = go(remote(fb.at[j, me_e], fb.at[j, me_e], near_send.at[j], near_recv.at[j], partner, me_p))
        if j == 0:
            own[pieces].wait()
            tangents = [
                go(remote(tg.at[me_p], tg.at[me_p], tg_send.at[d], tg_recv.at[d],
                          me_e, lax.rem(me_p + d, n_p)))
                for d in range(1, n_p)
            ]

    forwards = {}

    def forward(j):
        for d in order:
            gather[j, d].wait_recv()
            at = back(d) * 2 + core
            forwards[j, d] = go(remote(fb.at[j, at], fb.at[j, at], fw_send.at[j, d], fw_recv.at[j, d],
                                       partner, me_p))

    for copy in loads:
        copy.wait()
    block = TILE

    used_rows[...] = jnp.zeros_like(used_rows)
    used_rows[: mask.shape[0], :] = mask[...].astype(jnp.float32)
    used_cols[...] = used_rows[...].T

    def weigh(r, _):
        at = pl.ds(pl.multiple_of(r * block, block), block)
        used = used_cols[at, :]
        for t in range(cols // TILE):
            here = pl.ds(t * TILE, TILE)
            tr = trans[at, here].astype(jnp.float32)
            weights[at, here] = (
                tr * tr * ivar[at, here].astype(jnp.float32)
                * jnp.broadcast_to(used[:, t:t + 1], (block, TILE)))
        return 0

    lax.fori_loop(0, rows // block, weigh, 0)
    coef_t[...] = coef[...].T

    for copy in tangents:
        copy.wait_recv()
    tang[...] = tg[...].reshape(rank, rows).T

    def first_term(r, _):
        at = pl.ds(pl.multiple_of(r * block, block), block)
        for j in range(pieces):
            here = pl.ds(j * width, width)
            moved[at, here] = jnp.dot(tang[at, :], basis[:, here], preferred_element_type=jnp.float32)
        return 0

    lax.fori_loop(0, rows // block, first_term, 0)

    def work(j):
        here = pl.ds(j * width, width)
        near[j].wait_recv()
        for d in range(1, chips):
            forwards[j, d].wait_recv()
        full = fb[j].reshape(rank, width)

        def second_term(r, _):
            at = pl.ds(pl.multiple_of(r * block, block), block)
            total = moved[at, here] + jnp.dot(coef[at, :], full, preferred_element_type=jnp.float32)
            wt[at, :] = (weights[at, here] * total).astype(jnp.bfloat16)
            return 0

        lax.fori_loop(0, rows // block, second_term, 0)
        term = jnp.dot(coef_t[...], wt[...], preferred_element_type=jnp.float32)
        part[j] = term.reshape(chips, 2, rank // n_e, width)
        copy = go(remote(part.at[j, :, 1 - core], swap.at[j], swap_send.at[j], swap_recv.at[j], partner, me_p))
        cterm = lax.dot_general(
            basis[:, here], wt[...], (((1,), (1,)), ((), ())), preferred_element_type=jnp.float32
        ).reshape(n_p, cb, rows)
        cpart[...] = cterm if j == 0 else cpart[...] + cterm
        return copy

    def scatter(j, copy):
        copy.wait_recv()
        out = []
        for d in range(1, chips):
            to = over(d)
            value, factor = scaled(part[j, to, core] + swap[j, to])
            rs_out[j, d] = value
            rs_fac_out[j, d] = factor
            out.append(go(remote(rs_out.at[j, d], rs_in.at[j, d], rs_send.at[j, d], rs_recv.at[j, d],
                                 to * 2 + core, me_p)))
            out.append(go(remote(rs_fac_out.at[j, d], rs_fac_in.at[j, d], rsf_send.at[j, d], rsf_recv.at[j, d],
                                 to * 2 + core, me_p)))
        return out

    swaps, scatters = {}, {}
    forward(0)
    for j in range(pieces):
        swaps[j] = work(j)
        if j + 1 < pieces:
            forward(j + 1)
        else:
            csent = []
            for d in range(1, n_p):
                to = lax.rem(me_p + d, n_p)
                value, factor = scaled(cpart[to])
                cs_out[d] = value
                cs_fac_out[d] = factor
                csent.append(go(remote(cs_out.at[d], cs_in.at[d], cs_send.at[d], cs_recv.at[d], me_e, to)))
                csent.append(go(remote(cs_fac_out.at[d], cs_fac_in.at[d], csf_send.at[d], csf_recv.at[d], me_e, to)))
        scatters[j] = scatter(j, swaps[j])

    for copy in csent:
        copy.wait_recv()
    total = cpart[me_p]
    for d in range(1, n_p):
        total = total + restored(cs_in[d], cs_fac_in[d])
    cout[...] = total * (1.0 / math.sqrt(cols * n_p))

    for j in range(pieces):
        for copy in scatters[j]:
            copy.wait_recv()
        total = part[j, chip, core] + swap[j, chip]
        for d in range(1, chips):
            total = total + restored(rs_in[j, d], rs_fac_in[j, d])
        bout[:, j * width:(j + 1) * width] = total * (1.0 / math.sqrt(rows * n_e))

    for copy in sends:
        copy.wait_send()


def finish(by_pixels, by_exposures, coef_sum, basis_sum, coef_grad, basis_grad):
    coef_grad[...] = coef_sum[...] * by_pixels
    basis_grad[...] = basis_sum[...] * by_exposures


def drain(a, b, x, y, sem):
    c0 = pltpu.make_async_copy(a, x, sem.at[0])
    c1 = pltpu.make_async_copy(b, y, sem.at[1])
    c1.start()
    c0.start()
    c1.wait()
    c0.wait()


def body(n_e, n_p, *args):
    trans, ivar, mask, coef, basis, ctan, btan = args
    rows, cols = trans.shape
    rank = coef.shape[1]
    chips = n_e // 2
    rb, cb = rank // n_e, rank // n_p
    pieces = split_columns(cols)
    width = cols // pieces
    padded = -(-mask.shape[1] // TILE) * TILE
    f32, bf16 = jnp.float32, jnp.bfloat16
    dma = pltpu.SemaphoreType.DMA
    V = pltpu.VMEM
    coef_sum, basis_sum = pl.pallas_call(
        functools.partial(kernel, n_e, n_p, pieces),
        out_shape=(pltpu.VMEM((cb, rows), f32), pltpu.VMEM((rb, cols), f32)),
        in_specs=[pl.BlockSpec(memory_space=pl.ANY)] * 7,
        out_specs=(pl.BlockSpec(memory_space=pltpu.VMEM),) * 2,
        scratch_shapes=[
            V(trans.shape, bf16), V(ivar.shape, bf16), V(mask.shape[::-1], jnp.int32), V(coef.shape, bf16),
            V(basis.shape, bf16), V((n_p, cb, rows), bf16), V((pieces, n_e, rb, width), bf16),
            V((padded, rows), f32), V((rows, padded), f32),
            V((rows, rank), bf16), V((rank, rows), bf16), V((rows, cols), f32), V((rows, cols), f32),
            V((rows, width), bf16),
            V((pieces, chips, 2, rb, width), f32), V((pieces, chips, rb, width), f32),
            V((pieces, chips, rb, width), WIRE), V((pieces, chips, rb, width), WIRE),
            V((pieces, chips, 1, width), f32), V((pieces, chips, 1, width), f32),
            V((n_p, cb, rows), f32), V((n_p, cb, rows), WIRE), V((n_p, cb, rows), WIRE),
            V((n_p, 1, rows), f32), V((n_p, 1, rows), f32),
            dma((5,)), dma((pieces + 1,)),
            dma((n_p,)), dma((n_p,)), dma((pieces, chips)), dma((pieces, chips)),
            dma((pieces,)), dma((pieces,)), dma((pieces, chips)), dma((pieces, chips)),
            dma((pieces,)), dma((pieces,)), dma((pieces, chips)), dma((pieces, chips)),
            dma((pieces, chips)), dma((pieces, chips)),
            dma((n_p,)), dma((n_p,)), dma((n_p,)), dma((n_p,)),
        ],
        compiler_params=pltpu.CompilerParams(
            collective_id=0, has_side_effects=True, vmem_limit_bytes=56 * 1024 * 1024
        ),
    )(trans, ivar, mask.T, coef, basis, ctan.T, btan)
    coef_grad, basis_grad = pl.pallas_call(
        drain,
        out_shape=(jax.ShapeDtypeStruct((cb, rows), f32), jax.ShapeDtypeStruct((rb, cols), f32)),
        in_specs=[pl.BlockSpec(memory_space=pltpu.VMEM)] * 2,
        out_specs=(pl.BlockSpec(memory_space=pl.ANY),) * 2,
        scratch_shapes=[dma((2,))],
    )(pltpu.with_memory_space_constraint(coef_sum, pltpu.VMEM), pltpu.with_memory_space_constraint(basis_sum, pltpu.VMEM))
    return coef_grad.T, basis_grad


def solution(mesh):
    placed = (
        P("exp", "pix"),
        P("exp", "pix"),
        P("exp", "pix"),
        P("exp", None),
        P(None, "pix"),
        P("exp", "pix"),
        P("exp", "pix"),
    )
    return jax.shard_map(
        functools.partial(body, mesh.shape["exp"], mesh.shape["pix"]),
        mesh=mesh,
        in_specs=placed,
        out_specs=(P("exp", "pix"), P("exp", "pix")),
        check_vma=False,
    )
```

```python
import functools
import math

import jax
import jax.numpy as jnp
from jax import lax
from jax.experimental import pallas as pl
from jax.experimental.pallas import tpu as pltpu
from jax.sharding import PartitionSpec as P

TILE = 128
WIRE = jnp.int16
PIECES = 2
TOP = 32767.0
TINY = 1e-30
MESH = pl.DeviceIdType.MESH


def split_columns(cols):
    tiles = cols // (2 * TILE)
    pieces = min(PIECES, tiles)
    return [TILE * ((tiles + i) // pieces) for i in reversed(range(pieces))]


def scaled(x):
    peak = jnp.maximum(jnp.max(jnp.abs(x), axis=0, keepdims=True), TINY)
    return jnp.round(x * (TOP / peak)).astype(jnp.int32).astype(WIRE), peak * (1.0 / TOP)


def restored(value, factor):
    return value.astype(jnp.int32).astype(jnp.float32) * factor


def kernel(n_e, n_p, widths, trans_h, ivar_h, mask_h, coef_h, basis_h, ctan_h, btan_h, cout, bout, *scratch):
    scratch = list(scratch)

    def take(n=None):
        if n is None:
            return scratch.pop(0)
        return [scratch.pop(0) for _ in range(n)]

    pieces = len(widths)
    trans, ivar, mask, coef, basis, tg = take(6)
    fb, bo = take(pieces), take(pieces)
    used_rows, used_cols, tang, coef_t, weights, moved = take(6)
    wt, part, pin, rs_out, rs_in, rs_fac_out, rs_fac_in = (take(pieces) for _ in range(7))
    cpart, cswap, cs_out, cs_in, cs_fac_out, cs_fac_in = take(6)
    load_sem, own_sem, far_sem = take(3)
    tg_send, tg_recv, ag_send, ag_recv, fw_send, ex_send, ex_recv = take(7)
    pin_send, pin_recv, rs_send, rs_recv, rsf_send, rsf_recv = take(6)
    sw_send, sw_recv, cs_send, cs_recv, csf_send, csf_recv = take(6)
    assert not scratch
    rows, half = trans.shape[1:]
    rank = coef.shape[2]
    starts = [sum(widths[:j]) for j in range(pieces)]
    chips = n_e // 2
    cb = rank // n_p
    me_e, me_p = lax.axis_index("exp"), lax.axis_index("pix")
    core, chip = lax.rem(me_e, 2), me_e // 2
    across = 1 - core
    partner = chip * 2 + across

    def lanes(c, start, width):
        return pl.ds(pl.multiple_of(c * half + start, TILE), width)

    def remote(src, dst, send, recv, e, p):
        return pltpu.make_async_remote_copy(
            src_ref=src, dst_ref=dst, send_sem=send, recv_sem=recv,
            device_id=(e, p), device_id_type=MESH,
        )

    own, far = [], []
    for j in range(pieces):
        own.append(pltpu.make_async_copy(
            btan_h.at[:, lanes(core, starts[j], widths[j])], fb[j].at[chip, core], own_sem.at[j]))
        far.append(pltpu.make_async_copy(
            btan_h.at[:, lanes(across, starts[j], widths[j])], bo[j], far_sem.at[j]))
    own.append(pltpu.make_async_copy(ctan_h, tg.at[core, me_p], own_sem.at[pieces]))
    for copy in own[:pieces] + far + own[pieces:]:
        copy.start()
    mine = lanes(core, 0, half)
    loads = [
        pltpu.make_async_copy(src, dst, load_sem.at[i])
        for i, (src, dst) in enumerate((
            (trans_h.at[:, mine], trans.at[core]), (ivar_h.at[:, mine], ivar.at[core]), (mask_h, mask.at[core]),
            (coef_h, coef.at[core]), (basis_h.at[:, mine], basis)))
    ]
    for copy in loads:
        copy.start()

    barrier = pltpu.get_barrier_semaphore()
    for d in range(1, chips):
        for c in range(2):
            pl.semaphore_signal(barrier, inc=1, device_id=(lax.rem(chip + d, chips) * 2 + c, me_p), device_id_type=MESH)
    pl.semaphore_signal(barrier, inc=1, device_id=(partner, me_p), device_id_type=MESH)
    for d in range(1, n_p):
        pl.semaphore_signal(barrier, inc=1, device_id=(me_e, lax.rem(me_p + d, n_p)), device_id_type=MESH)
    pl.semaphore_wait(barrier, 2 * (chips - 1) + n_p)

    sends = []

    def go(copy):
        copy.start()
        sends.append(copy)
        return copy

    hub = chips == 4
    if hub:
        side = chip // 2
        end, inner = 3 * side, 1 + side
        far_end, far_inner = 3 - end, 3 - inner
        is_inner = chip == inner
        mate = jnp.where(is_inner, end, inner)
        targets = [far_inner, mate]
    else:
        targets = [lax.rem(chip + d, chips) for d in range(1, chips)]

    def send_own(j):
        mine, theirs = fb[j].at[chip, core], bo[j]
        for i, to in enumerate(targets):
            go(remote(mine, mine, ag_send.at[j, i, 0], ag_recv.at[j, chip, core], to * 2 + core, me_p))
            go(remote(theirs, mine, ag_send.at[j, i, 1], ag_recv.at[j, chip, core], to * 2 + across, me_p))
        go(remote(theirs, mine, ag_send.at[j, chips - 1, 1], ag_recv.at[j, chip, core], partner, me_p))

    def arrived(j, k, c):
        block = fb[j].at[k, c]
        remote(block, block, ag_send.at[j, 0, 0], ag_recv.at[j, k, c], partner, me_p).wait_recv()

    def pass_copy(j, i):
        k = (far_inner, far_end)[i]
        return remote(fb[j].at[k], fb[j].at[k], fw_send.at[j, i], ag_recv.at[j, k, 0], end * 2 + core, me_p)

    def pass_on(j):
        if not hub:
            return

        @pl.when(is_inner)
        def _():
            for i in range(2):
                k = (far_inner, far_end)[i]
                arrived(j, k, 0)
                arrived(j, k, 1)
                pass_copy(j, i).start()

    def complete(j):
        arrived(j, chip, across)
        if not hub:
            for to in targets:
                arrived(j, to, 0)
                arrived(j, to, 1)
            return
        arrived(j, mate, 0)
        arrived(j, mate, 1)

        @pl.when(jnp.logical_not(is_inner))
        def _():
            pass_copy(j, 0).wait_recv()
            pass_copy(j, 1).wait_recv()

    for j in range(pieces):
        own[j].wait()
        far[j].wait()
        send_own(j)
    own[pieces].wait()
    tangents = [
        go(remote(tg.at[core, me_p], tg.at[core, me_p], tg_send.at[d], tg_recv.at[d],
                  me_e, lax.rem(me_p + d, n_p)))
        for d in range(1, n_p)
    ]
    theirs = lanes(across, 0, half)
    exchanged = [
        go(remote(src, dst, ex_send.at[i], ex_recv.at[i], partner, me_p))
        for i, (src, dst) in enumerate((
            (mask_h, mask.at[core]), (coef_h, coef.at[core]),
            (trans_h.at[:, theirs], trans.at[core]), (ivar_h.at[:, theirs], ivar.at[core])))
    ]
    block = TILE
    tiles = half // TILE
    used_rows[...] = jnp.zeros_like(used_rows)

    def weigh_all(c):
        used = mask[c].astype(jnp.float32)
        used_rows[c, :tiles, :] = jnp.where(core == 0, used[:tiles], used[tiles:])
        used_cols[c] = used_rows[c].T

        def weigh(r, _):
            at = pl.ds(pl.multiple_of(r * block, block), block)
            used = used_cols[c, at, :]
            for t in range(tiles):
                here = pl.ds(t * TILE, TILE)
                tr = trans[c, at, here].astype(jnp.float32)
                weights[c, at, here] = (
                    tr * tr * ivar[c, at, here].astype(jnp.float32)
                    * jnp.broadcast_to(used[:, t:t + 1], (block, TILE)))
            return 0

        lax.fori_loop(0, rows // block, weigh, 0)
        coef_t[c] = coef[c].T


    def first(c):
        tang[c] = tg[c].reshape(rank, rows).T

        def first_term(r, _):
            at = pl.ds(pl.multiple_of(r * block, block), block)
            for j in range(pieces):
                here = pl.ds(starts[j], widths[j])
                moved[c, at, here] = jnp.dot(tang[c, at, :], basis[:, here], preferred_element_type=jnp.float32)
            return 0

        lax.fori_loop(0, rows // block, first_term, 0)

    for copy in loads:
        copy.wait()
    weigh_all(core)
    pass_on(0)
    for copy in tangents:
        copy.wait_recv()
    other_tangent = go(remote(tg.at[core], tg.at[core], ex_send.at[4], ex_recv.at[4], partner, me_p))
    first(core)
    for j in range(1, pieces):
        pass_on(j)
    for copy in exchanged:
        copy.wait_recv()
    weigh_all(across)
    other_tangent.wait_recv()
    first(across)

    def other(i, me):
        return i + (i >= me).astype(jnp.int32)

    def slot_at(to, me):
        return jnp.where(me > to, me - 1, me)

    def swap_copy(to):
        return remote(cpart.at[across, to], cswap.at[to], sw_send.at[to], sw_recv.at[to], partner, me_p)

    def work(j):
        width = widths[j]
        here = pl.ds(starts[j], width)
        complete(j)
        full = fb[j][...].reshape(rank, width)
        for c in range(2):
            total = moved[c, :, here] + jnp.dot(coef[c], full, preferred_element_type=jnp.float32)
            wt[j][c] = (weights[c, :, here] * total).astype(jnp.bfloat16)

        def coef_part():
            for c in range(2):
                cterm = lax.dot_general(
                    basis[:, here], wt[j][c], (((1,), (1,)), ((), ())), preferred_element_type=jnp.float32
                ).reshape(n_p, cb, rows)
                cpart[c] = cterm if j == 0 else cpart[c] + cterm

        last = j + 1 == pieces
        if last:
            coef_part()
            for i in range(n_p - 1):
                swap_copy(other(i, me_p)).start()
            swap_copy(me_p).start()
        term = (jnp.dot(coef_t[0], wt[j][0], preferred_element_type=jnp.float32)
                + jnp.dot(coef_t[1], wt[j][1], preferred_element_type=jnp.float32))
        part[j][...] = term.reshape(chips, 2, rank // n_e, width)
        scatter(j)
        if not last:
            coef_part()

    def rs_copies(j, i, c, to, slot, at):
        return (remote(rs_out[j].at[i, c], rs_in[j].at[slot, at], rs_send.at[j, i, c], rs_recv.at[j, slot, at],
                       to * 2 + c, me_p),
                remote(rs_fac_out[j].at[i, c], rs_fac_in[j].at[slot, at], rsf_send.at[j, i, c], rsf_recv.at[j, slot, at],
                       to * 2 + c, me_p))

    def scatter(j):
        for i in range(chips - 1):
            to = other(i, chip)
            slot = slot_at(to, chip)
            for c in range(2):
                value, factor = scaled(part[j][to, c])
                rs_out[j][i, c] = value
                rs_fac_out[j][i, c] = factor
                for copy in rs_copies(j, i, c, to, slot, core):
                    go(copy)
        go(remote(part[j].at[chip, across], pin[j], pin_send.at[j], pin_recv.at[j], partner, me_p))

    def gathered(j):
        remote(pin[j], pin[j], pin_send.at[j], pin_recv.at[j], partner, me_p).wait_recv()
        totals = [jnp.where(core == h, part[j][chip, core], pin[j][...]) for h in range(2)]
        for i in range(chips - 1):
            for h in range(2):
                for copy in rs_copies(j, i, 0, chip, i, h):
                    copy.wait_recv()
                totals[h] = totals[h] + restored(rs_in[j][i, h], rs_fac_in[j][i, h])
        for h in range(2):
            at = h * half + starts[j]
            bout[:, at:at + widths[j]] = totals[h] * (1.0 / math.sqrt(rows * n_e))

    for j in range(pieces):
        work(j)

    for i in range(n_p - 1):
        to = other(i, me_p)
        slot = slot_at(to, me_p)
        swap_copy(to).wait_recv()
        value, factor = scaled(cpart[core, to] + cswap[to])
        cs_out[i] = value
        cs_fac_out[i] = factor
        go(remote(cs_out.at[i], cs_in.at[slot], cs_send.at[i], cs_recv.at[slot], me_e, to))
        go(remote(cs_fac_out.at[i], cs_fac_in.at[slot], csf_send.at[i], csf_recv.at[slot], me_e, to))
    swap_copy(me_p).wait_recv()

    for j in range(pieces - 1):
        gathered(j)
    gathered(pieces - 1)
    total = cpart[core, me_p] + cswap[me_p]
    for i in range(n_p - 1):
        remote(cs_out.at[i], cs_in.at[i], cs_send.at[i], cs_recv.at[i], partner, me_p).wait_recv()
        remote(cs_fac_out.at[i], cs_fac_in.at[i], csf_send.at[i], csf_recv.at[i], partner, me_p).wait_recv()
        total = total + restored(cs_in[i], cs_fac_in[i])
    cout[...] = total * (1.0 / math.sqrt(half * 2 * n_p))

    for copy in sends:
        copy.wait_send()
    for i in range(n_p):
        swap_copy(i).wait_send()
    if hub:
        @pl.when(is_inner)
        def _():
            for j in range(pieces):
                pass_copy(j, 0).wait_send()
                pass_copy(j, 1).wait_send()


def drain(a, b, x, y, sem):
    c0 = pltpu.make_async_copy(a, x, sem.at[0])
    c1 = pltpu.make_async_copy(b, y, sem.at[1])
    c1.start()
    c0.start()
    c1.wait()
    c0.wait()


def body(n_e, n_p, *args):
    trans, ivar, mask, coef, basis, ctan, btan = args
    rows, cols = trans.shape
    rank = coef.shape[1]
    chips = n_e // 2
    rb, cb = rank // n_e, rank // n_p
    widths = split_columns(cols)
    pieces = len(widths)
    half = cols // 2
    padded = -(-(half // TILE) // TILE) * TILE
    f32, bf16 = jnp.float32, jnp.bfloat16
    dma = pltpu.SemaphoreType.DMA
    V = pltpu.VMEM

    def each(shape, dtype):
        return [V(tuple(w if v is None else v for v in shape), dtype) for w in widths]

    coef_sum, basis_sum = pl.pallas_call(
        functools.partial(kernel, n_e, n_p, widths),
        out_shape=(pltpu.VMEM((cb, rows), f32), pltpu.VMEM((rb, cols), f32)),
        in_specs=[pl.BlockSpec(memory_space=pl.ANY)] * 7,
        out_specs=(pl.BlockSpec(memory_space=pltpu.VMEM),) * 2,
        scratch_shapes=[
            V((2, rows, half), bf16), V((2, rows, half), bf16), V((2, *mask.shape[::-1]), jnp.int32),
            V((2, rows, rank), bf16), V((rank, half), bf16), V((2, n_p, cb, rows), bf16),
            *each((chips, 2, rb, None), bf16), *each((rb, None), bf16),
            V((2, padded, rows), f32), V((2, rows, padded), f32),
            V((2, rows, rank), bf16), V((2, rank, rows), bf16), V((2, rows, half), f32), V((2, rows, half), f32),
            *each((2, rows, None), bf16),
            *each((chips, 2, rb, None), f32), *each((rb, None), f32),
            *each((chips - 1, 2, rb, None), WIRE), *each((chips - 1, 2, rb, None), WIRE),
            *each((chips - 1, 2, 1, None), f32), *each((chips - 1, 2, 1, None), f32),
            V((2, n_p, cb, rows), f32), V((n_p, cb, rows), f32), V((n_p, cb, rows), WIRE), V((n_p, cb, rows), WIRE),
            V((n_p, 1, rows), f32), V((n_p, 1, rows), f32),
            dma((5,)), dma((pieces + 1,)), dma((pieces,)),
            dma((n_p,)), dma((n_p,)), dma((pieces, chips, 2)), dma((pieces, chips, 2)), dma((pieces, 2)),
            dma((5,)), dma((5,)),
            dma((pieces,)), dma((pieces,)), dma((pieces, chips, 2)), dma((pieces, chips, 2)),
            dma((pieces, chips, 2)), dma((pieces, chips, 2)),
            dma((n_p,)), dma((n_p,)), dma((n_p,)), dma((n_p,)), dma((n_p,)), dma((n_p,)),
        ],
        compiler_params=pltpu.CompilerParams(
            collective_id=0, has_side_effects=True, vmem_limit_bytes=56 * 1024 * 1024
        ),
    )(trans, ivar, mask.T, coef, basis, ctan.T, btan)
    coef_grad, basis_grad = pl.pallas_call(
        drain,
        out_shape=(jax.ShapeDtypeStruct((cb, rows), f32), jax.ShapeDtypeStruct((rb, cols), f32)),
        in_specs=[pl.BlockSpec(memory_space=pltpu.VMEM)] * 2,
        out_specs=(pl.BlockSpec(memory_space=pl.ANY),) * 2,
        scratch_shapes=[dma((2,))],
    )(*[pltpu.with_memory_space_constraint(v, pltpu.VMEM) for v in (coef_sum, basis_sum)])
    return coef_grad.T, basis_grad


def solution(mesh):
    placed = (
        P("exp", "pix"),
        P("exp", "pix"),
        P("exp", "pix"),
        P("exp", None),
        P(None, "pix"),
        P("exp", "pix"),
        P("exp", "pix"),
    )
    return jax.shard_map(
        functools.partial(body, mesh.shape["exp"], mesh.shape["pix"]),
        mesh=mesh,
        in_specs=placed,
        out_specs=(P("exp", "pix"), P("exp", "pix")),
        check_vma=False,
    )
```

```python
import functools
import math

import jax
import jax.numpy as jnp
from jax import lax
from jax.experimental import pallas as pl
from jax.experimental.pallas import tpu as pltpu
from jax.sharding import PartitionSpec as P

TILE = 128
WIRE = jnp.int16
TOP = 32767.0
TINY = 1e-30
MESH = pl.DeviceIdType.MESH

def split_columns(cols):
    tiles = cols // (2 * TILE)
    first = tiles // 3
    return [TILE * v for v in (first, tiles - first) if v]


def scaled(x):
    peak = jnp.maximum(jnp.max(jnp.abs(x), axis=0, keepdims=True), TINY)
    return jnp.round(x * (TOP / peak)).astype(jnp.int32).astype(WIRE), peak * (1.0 / TOP)


def restored(value, factor):
    return value.astype(jnp.int32).astype(jnp.float32) * factor


def kernel(n_e, n_p, widths, trans_h, ivar_h, mask_h, coef_h, basis_h, ctan_h, btan_h, cout, bout, *scratch):
    scratch = list(scratch)

    def take(n=None):
        if n is None:
            return scratch.pop(0)
        return [scratch.pop(0) for _ in range(n)]

    pieces = len(widths)
    trans, ivar, mask, coef, basis, tg = take(6)
    fb, bo = take(pieces), take(pieces)
    used_rows, used_cols, tang, coef_t, weights, moved = take(6)
    wt, part, pin, rs_out, rs_in, rs_fac_out, rs_fac_in = (take(pieces) for _ in range(7))
    cpart, cswap, cs_out, cs_in, cs_fac_out, cs_fac_in = take(6)
    load_sem, own_sem, far_sem = take(3)
    tg_send, tg_recv, ag_send, ag_recv, fw_send, ex_send, ex_recv = take(7)
    pin_send, pin_recv, rs_send, rs_recv, rsf_send, rsf_recv = take(6)
    sw_send, sw_recv, cs_send, cs_recv, csf_send, csf_recv = take(6)
    assert not scratch
    rows, half = trans.shape[1:]
    rank = coef.shape[2]
    starts = [sum(widths[:j]) for j in range(pieces)]
    chips = n_e // 2
    cb = rank // n_p
    me_e, me_p = lax.axis_index("exp"), lax.axis_index("pix")
    core, chip = lax.rem(me_e, 2), me_e // 2
    across = 1 - core
    partner = chip * 2 + across

    def lanes(c, start, width):
        return pl.ds(pl.multiple_of(c * half + start, TILE), width)

    def remote(src, dst, send, recv, e, p):
        return pltpu.make_async_remote_copy(
            src_ref=src, dst_ref=dst, send_sem=send, recv_sem=recv,
            device_id=(e, p), device_id_type=MESH,
        )

    own, far = [], []
    for j in range(pieces):
        own.append(pltpu.make_async_copy(
            btan_h.at[:, lanes(core, starts[j], widths[j])], fb[j].at[chip, core], own_sem.at[j]))
        far.append(pltpu.make_async_copy(
            btan_h.at[:, lanes(across, starts[j], widths[j])], bo[j], far_sem.at[j]))
    own.append(pltpu.make_async_copy(ctan_h, tg.at[core, me_p], own_sem.at[pieces]))
    for copy in own[:pieces] + far + own[pieces:]:
        copy.start()
    mine = lanes(core, 0, half)
    loads = [
        pltpu.make_async_copy(src, dst, load_sem.at[i])
        for i, (src, dst) in enumerate((
            (trans_h.at[:, mine], trans.at[core]), (ivar_h.at[:, mine], ivar.at[core]), (mask_h, mask.at[core]),
            (coef_h, coef.at[core]), (basis_h.at[:, mine], basis)))
    ]
    for copy in loads:
        copy.start()

    barrier = pltpu.get_barrier_semaphore()
    for d in range(1, chips):
        for c in range(2):
            pl.semaphore_signal(barrier, inc=1, device_id=(lax.rem(chip + d, chips) * 2 + c, me_p), device_id_type=MESH)
    pl.semaphore_signal(barrier, inc=1, device_id=(partner, me_p), device_id_type=MESH)
    for d in range(1, n_p):
        pl.semaphore_signal(barrier, inc=1, device_id=(me_e, lax.rem(me_p + d, n_p)), device_id_type=MESH)
    pl.semaphore_wait(barrier, 2 * (chips - 1) + n_p)

    sends = []

    def go(copy):
        copy.start()
        sends.append(copy)
        return copy

    hub = chips == 4
    if hub:
        side = chip // 2
        end, inner = 3 * side, 1 + side
        far_end, far_inner = 3 - end, 3 - inner
        is_inner = chip == inner
        mate = jnp.where(is_inner, end, inner)
        targets = [far_inner, mate]
    else:
        targets = [lax.rem(chip + d, chips) for d in range(1, chips)]

    def send_to(j, i, to):
        mine, theirs = fb[j].at[chip, core], bo[j]
        return (remote(mine, mine, ag_send.at[j, i, 0], ag_recv.at[j, chip, core], to * 2 + core, me_p),
                remote(theirs, mine, ag_send.at[j, i, 1], ag_recv.at[j, chip, core], to * 2 + across, me_p))

    def send_own(j):
        for i, to in enumerate(targets):
            for copy in send_to(j, i, to):
                go(copy)
        go(remote(bo[j], fb[j].at[chip, core], ag_send.at[j, chips - 1, 1], ag_recv.at[j, chip, core], partner, me_p))

    def arrived(j, k, c):
        block = fb[j].at[k, c]
        remote(block, block, ag_send.at[j, 0, 0], ag_recv.at[j, k, c], partner, me_p).wait_recv()

    def pass_copy(j, i):
        k = (far_inner, far_end)[i]
        return remote(fb[j].at[k], fb[j].at[k], fw_send.at[j, i], ag_recv.at[j, k, 0], end * 2 + core, me_p)

    def pass_on(j):
        if not hub:
            return

        @pl.when(is_inner)
        def _():
            for i in range(2):
                k = (far_inner, far_end)[i]
                arrived(j, k, 0)
                arrived(j, k, 1)
                pass_copy(j, i).start()

    def complete(j):
        arrived(j, chip, across)
        if not hub:
            for to in targets:
                arrived(j, to, 0)
                arrived(j, to, 1)
            return
        arrived(j, mate, 0)
        arrived(j, mate, 1)

        @pl.when(jnp.logical_not(is_inner))
        def _():
            for i in range(2):
                pass_copy(j, i).wait_recv()

    for j in range(pieces):
        own[j].wait()
        far[j].wait()
        send_own(j)
    own[pieces].wait()
    tangents = [
        go(remote(tg.at[core, me_p], tg.at[core, me_p], tg_send.at[d], tg_recv.at[d],
                  me_e, lax.rem(me_p + d, n_p)))
        for d in range(1, n_p)
    ]
    theirs = lanes(across, 0, half)
    exchanged = [
        go(remote(src, dst, ex_send.at[i], ex_recv.at[i], partner, me_p))
        for i, (src, dst) in enumerate((
            (mask_h, mask.at[core]), (coef_h, coef.at[core]),
            (trans_h.at[:, theirs], trans.at[core]), (ivar_h.at[:, theirs], ivar.at[core])))
    ]
    block = TILE
    tiles = half // TILE
    used_rows[...] = jnp.zeros_like(used_rows)

    def weigh_all(c):
        used = mask[c].astype(jnp.float32)
        used_rows[c, :tiles, :] = jnp.where(core == 0, used[:tiles], used[tiles:])
        used_cols[c] = used_rows[c].T

        def weigh(r, _):
            at = pl.ds(pl.multiple_of(r * block, block), block)
            used = used_cols[c, at, :]
            for t in range(tiles):
                here = pl.ds(t * TILE, TILE)
                tr = trans[c, at, here].astype(jnp.float32)
                weights[c, at, here] = (
                    tr * tr * ivar[c, at, here].astype(jnp.float32)
                    * jnp.broadcast_to(used[:, t:t + 1], (block, TILE)))
            return 0

        lax.fori_loop(0, rows // block, weigh, 0)
        coef_t[c] = coef[c].T

    def first(c):
        tang[c] = tg[c].reshape(rank, rows).T

        def first_term(r, _):
            at = pl.ds(pl.multiple_of(r * block, block), block)
            for j in range(pieces):
                here = pl.ds(starts[j], widths[j])
                moved[c, at, here] = jnp.dot(tang[c, at, :], basis[:, here], preferred_element_type=jnp.float32)
            return 0

        lax.fori_loop(0, rows // block, first_term, 0)

    for copy in loads:
        copy.wait()
    weigh_all(core)
    pass_on(0)
    for copy in tangents:
        copy.wait_recv()
    other_tangent = go(remote(tg.at[core], tg.at[core], ex_send.at[4], ex_recv.at[4], partner, me_p))
    first(core)
    for j in range(1, pieces):
        pass_on(j)
    for copy in exchanged:
        copy.wait_recv()
    weigh_all(across)
    other_tangent.wait_recv()
    first(across)

    def other(i, me):
        return i + (i >= me).astype(jnp.int32)

    def slot_at(to, me):
        return jnp.where(me > to, me - 1, me)

    def swap_copy(to):
        return remote(cpart.at[across, to], cswap.at[to], sw_send.at[to], sw_recv.at[to], partner, me_p)

    def start_swap():
        for i in range(n_p - 1):
            swap_copy(other(i, me_p)).start()
        swap_copy(me_p).start()

    def work(j):
        width = widths[j]
        here = pl.ds(starts[j], width)
        last = j + 1 == pieces
        complete(j)
        full = fb[j][...].reshape(rank, width)

        def second(c):
            total = moved[c, :, here] + jnp.dot(coef[c], full, preferred_element_type=jnp.float32)
            wt[j][c] = (weights[c, :, here] * total).astype(jnp.bfloat16)

        def coef_part(c):
            cterm = lax.dot_general(
                basis[:, here], wt[j][c], (((1,), (1,)), ((), ())), preferred_element_type=jnp.float32
            ).reshape(n_p, cb, rows)
            cpart[c] = cterm if j == 0 else cpart[c] + cterm

        if last:
            second(across)
            coef_part(across)
            start_swap()
            second(core)
        else:
            second(0)
            second(1)
        term = (jnp.dot(coef_t[0], wt[j][0], preferred_element_type=jnp.float32)
                + jnp.dot(coef_t[1], wt[j][1], preferred_element_type=jnp.float32))
        part[j][...] = term.reshape(chips, 2, rank // n_e, width)
        scatter(j)
        if not last:
            coef_part(0)
            coef_part(1)
        else:
            coef_part(core)

    def rs_joint(j, i, to, slot):
        return (remote(rs_out[j].at[i], rs_in[j].at[slot], rs_send.at[j, i, 0], rs_recv.at[j, slot, 0],
                       to * 2 + core, me_p),
                remote(rs_fac_out[j].at[i], rs_fac_in[j].at[slot], rsf_send.at[j, i, 0], rsf_recv.at[j, slot, 0],
                       to * 2 + core, me_p))

    def rs_copies(j, i, c, to, slot, at):
        return (remote(rs_out[j].at[i, c], rs_in[j].at[slot, at], rs_send.at[j, i, c], rs_recv.at[j, slot, at],
                       to * 2 + c, me_p),
                remote(rs_fac_out[j].at[i, c], rs_fac_in[j].at[slot, at], rsf_send.at[j, i, c], rsf_recv.at[j, slot, at],
                       to * 2 + c, me_p))

    merged = [j + 1 < pieces for j in range(pieces)]

    def put(j, i, c, total):
        value, factor = scaled(total)
        rs_out[j][i, c] = value
        rs_fac_out[j][i, c] = factor

    def scatter(j):
        for i in range(chips - 1):
            to = other(i, chip)
            slot = slot_at(to, chip)
            for c in range(2):
                put(j, i, c, part[j][to, c])
                if not merged[j]:
                    for copy in rs_copies(j, i, c, to, slot, core):
                        go(copy)
            if merged[j]:
                for copy in rs_joint(j, i, to, slot):
                    go(copy)
        if not merged[j]:
            go(remote(part[j].at[chip, across], pin[j], pin_send.at[j], pin_recv.at[j], partner, me_p))

    def reduced(j):
        if not merged[j]:
            return
        totals = [part[j][chip, c] for c in range(2)]
        for i in range(chips - 1):
            for copy in rs_joint(j, i, chip, i):
                copy.wait_recv()
            for c in range(2):
                totals[c] = totals[c] + restored(rs_in[j][i, c], rs_fac_in[j][i, c])
        for c in range(2):
            part[j][chip, c] = totals[c]
        go(remote(part[j].at[chip, across], pin[j], pin_send.at[j], pin_recv.at[j], partner, me_p))

    def gathered(j):
        remote(pin[j], pin[j], pin_send.at[j], pin_recv.at[j], partner, me_p).wait_recv()
        totals = [jnp.where(core == h, part[j][chip, core], pin[j][...]) for h in range(2)]
        for i in range(0 if merged[j] else chips - 1):
            for h in range(2):
                for copy in rs_copies(j, i, 0, chip, i, h):
                    copy.wait_recv()
                totals[h] = totals[h] + restored(rs_in[j][i, h], rs_fac_in[j][i, h])
        for h in range(2):
            at = h * half + starts[j]
            bout[:, at:at + widths[j]] = totals[h] * (1.0 / math.sqrt(rows * n_e))

    for j in range(pieces):
        work(j)

    for i in range(n_p - 1):
        to = other(i, me_p)
        slot = slot_at(to, me_p)
        swap_copy(to).wait_recv()
        value, factor = scaled(cpart[core, to] + cswap[to])
        cs_out[i] = value
        cs_fac_out[i] = factor
        go(remote(cs_out.at[i], cs_in.at[slot], cs_send.at[i], cs_recv.at[slot], me_e, to))
        go(remote(cs_fac_out.at[i], cs_fac_in.at[slot], csf_send.at[i], csf_recv.at[slot], me_e, to))
    swap_copy(me_p).wait_recv()

    for j in range(pieces):
        reduced(j)
    for j in range(pieces):
        gathered(j)
    total = cpart[core, me_p] + cswap[me_p]
    for i in range(n_p - 1):
        remote(cs_out.at[i], cs_in.at[i], cs_send.at[i], cs_recv.at[i], partner, me_p).wait_recv()
        remote(cs_fac_out.at[i], cs_fac_in.at[i], csf_send.at[i], csf_recv.at[i], partner, me_p).wait_recv()
        total = total + restored(cs_in[i], cs_fac_in[i])
    cout[...] = total * (1.0 / math.sqrt(half * 2 * n_p))

    for copy in sends:
        copy.wait_send()
    for i in range(n_p):
        swap_copy(i).wait_send()
    if hub:
        @pl.when(is_inner)
        def _():
            for j in range(pieces):
                for i in range(2):
                    pass_copy(j, i).wait_send()


def drain(a, b, x, y, sem):
    c0 = pltpu.make_async_copy(a, x, sem.at[0])
    c1 = pltpu.make_async_copy(b, y, sem.at[1])
    c1.start()
    c0.start()
    c1.wait()
    c0.wait()


def body(n_e, n_p, *args):
    trans, ivar, mask, coef, basis, ctan, btan = args
    rows, cols = trans.shape
    rank = coef.shape[1]
    chips = n_e // 2
    rb, cb = rank // n_e, rank // n_p
    widths = split_columns(cols)
    pieces = len(widths)
    half = cols // 2
    padded = -(-(half // TILE) // TILE) * TILE
    f32, bf16 = jnp.float32, jnp.bfloat16
    dma = pltpu.SemaphoreType.DMA
    V = pltpu.VMEM

    def each(shape, dtype):
        return [V(tuple(w if v is None else v for v in shape), dtype) for w in widths]

    coef_sum, basis_sum = pl.pallas_call(
        functools.partial(kernel, n_e, n_p, widths),
        out_shape=(pltpu.VMEM((cb, rows), f32), pltpu.VMEM((rb, cols), f32)),
        in_specs=[pl.BlockSpec(memory_space=pl.ANY)] * 7,
        out_specs=(pl.BlockSpec(memory_space=pltpu.VMEM),) * 2,
        scratch_shapes=[
            V((2, rows, half), bf16), V((2, rows, half), bf16), V((2, *mask.shape[::-1]), jnp.int32),
            V((2, rows, rank), bf16), V((rank, half), bf16), V((2, n_p, cb, rows), bf16),
            *each((chips, 2, rb, None), bf16), *each((rb, None), bf16),
            V((2, padded, rows), f32), V((2, rows, padded), f32),
            V((2, rows, rank), bf16), V((2, rank, rows), bf16), V((2, rows, half), f32), V((2, rows, half), f32),
            *each((2, rows, None), bf16),
            *each((chips, 2, rb, None), f32), *each((rb, None), f32),
            *each((chips - 1, 2, rb, None), WIRE), *each((chips - 1, 2, rb, None), WIRE),
            *each((chips - 1, 2, 1, None), f32), *each((chips - 1, 2, 1, None), f32),
            V((2, n_p, cb, rows), f32), V((n_p, cb, rows), f32), V((n_p, cb, rows), WIRE), V((n_p, cb, rows), WIRE),
            V((n_p, 1, rows), f32), V((n_p, 1, rows), f32),
            dma((5,)), dma((pieces + 1,)), dma((pieces,)),
            dma((n_p,)), dma((n_p,)), dma((pieces, chips, 2)), dma((pieces, chips, 2)), dma((pieces, 2)),
            dma((5,)), dma((5,)),
            dma((pieces,)), dma((pieces,)), dma((pieces, chips, 2)), dma((pieces, chips, 2)),
            dma((pieces, chips, 2)), dma((pieces, chips, 2)),
            dma((n_p,)), dma((n_p,)), dma((n_p,)), dma((n_p,)), dma((n_p,)), dma((n_p,)),
        ],
        compiler_params=pltpu.CompilerParams(
            collective_id=0, has_side_effects=True, vmem_limit_bytes=56 * 1024 * 1024
        ),
    )(trans, ivar, mask.T, coef, basis, ctan.T, btan)
    coef_grad, basis_grad = pl.pallas_call(
        drain,
        out_shape=(jax.ShapeDtypeStruct((cb, rows), f32), jax.ShapeDtypeStruct((rb, cols), f32)),
        in_specs=[pl.BlockSpec(memory_space=pltpu.VMEM)] * 2,
        out_specs=(pl.BlockSpec(memory_space=pl.ANY),) * 2,
        scratch_shapes=[dma((2,))],
    )(*[pltpu.with_memory_space_constraint(v, pltpu.VMEM) for v in (coef_sum, basis_sum)])
    return coef_grad.T, basis_grad


def solution(mesh):
    placed = (
        P("exp", "pix"),
        P("exp", "pix"),
        P("exp", "pix"),
        P("exp", None),
        P(None, "pix"),
        P("exp", "pix"),
        P("exp", "pix"),
    )
    return jax.shard_map(
        functools.partial(body, mesh.shape["exp"], mesh.shape["pix"]),
        mesh=mesh,
        in_specs=placed,
        out_specs=(P("exp", "pix"), P("exp", "pix")),
        check_vma=False,
    )
```

```python
import functools
import math

import jax
import jax.numpy as jnp
from jax import lax
from jax.experimental import pallas as pl
from jax.experimental.pallas import tpu as pltpu
from jax.sharding import PartitionSpec as P

TILE = 128
WIRE = jnp.int16
TOP = 32767.0
TINY = 1e-30
MESH = pl.DeviceIdType.MESH

def split_columns(cols):
    tiles = cols // (2 * TILE)
    first = tiles // 3
    return [TILE * v for v in (first, tiles - first) if v]


def scaled(x):
    peak = jnp.maximum(jnp.max(jnp.abs(x), axis=0, keepdims=True), TINY)
    return jnp.round(x * (TOP / peak)).astype(jnp.int32).astype(WIRE), peak * (1.0 / TOP)


def restored(value, factor):
    return value.astype(jnp.int32).astype(jnp.float32) * factor


def kernel(n_e, n_p, widths, trans_h, ivar_h, mask_h, coef_h, basis_h, ctan_h, btan_h, cout, bout, *scratch):
    scratch = list(scratch)

    def take(n=None):
        if n is None:
            return scratch.pop(0)
        return [scratch.pop(0) for _ in range(n)]

    pieces = len(widths)
    trans, ivar, mask, coef, basis, tg = take(6)
    fb, bo = take(pieces), take(pieces)
    used_rows, used_cols, tang, coef_t, weights, moved = take(6)
    wt, part, pin, rs_out, rs_in, rs_fac_out, rs_fac_in = (take(pieces) for _ in range(7))
    cpart, cswap, cs_out, cs_in, cs_fac_out, cs_fac_in = take(6)
    load_sem, own_sem, far_sem = take(3)
    tg_send, tg_recv, ag_send, ag_recv, fw_send, ex_send, ex_recv = take(7)
    pin_send, pin_recv, rs_send, rs_recv, rsf_send, rsf_recv = take(6)
    sw_send, sw_recv, cs_send, cs_recv, csf_send, csf_recv = take(6)
    assert not scratch
    rows, half = trans.shape[1:]
    rank = coef.shape[2]
    starts = [sum(widths[:j]) for j in range(pieces)]
    chips = n_e // 2
    cb = rank // n_p
    me_e, me_p = lax.axis_index("exp"), lax.axis_index("pix")
    core, chip = lax.rem(me_e, 2), me_e // 2
    across = 1 - core
    partner = chip * 2 + across

    def lanes(c, start, width):
        return pl.ds(pl.multiple_of(c * half + start, TILE), width)

    def remote(src, dst, send, recv, e, p):
        return pltpu.make_async_remote_copy(
            src_ref=src, dst_ref=dst, send_sem=send, recv_sem=recv,
            device_id=(e, p), device_id_type=MESH,
        )

    own, far = [], []
    for j in range(pieces):
        own.append(pltpu.make_async_copy(
            btan_h.at[:, lanes(core, starts[j], widths[j])], fb[j].at[chip, core], own_sem.at[j]))
        far.append(pltpu.make_async_copy(
            btan_h.at[:, lanes(across, starts[j], widths[j])], bo[j], far_sem.at[j]))
    own.append(pltpu.make_async_copy(ctan_h, tg.at[core, me_p], own_sem.at[pieces]))
    for copy in own[:pieces] + far + own[pieces:]:
        copy.start()
    mine = lanes(core, 0, half)
    loads = [
        pltpu.make_async_copy(src, dst, load_sem.at[i])
        for i, (src, dst) in enumerate((
            (trans_h.at[:, mine], trans.at[core]), (ivar_h.at[:, mine], ivar.at[core]), (mask_h, mask.at[core]),
            (coef_h, coef.at[core]), (basis_h.at[:, mine], basis)))
    ]
    for copy in loads:
        copy.start()

    barrier = pltpu.get_barrier_semaphore()
    for d in range(1, chips):
        for c in range(2):
            pl.semaphore_signal(barrier, inc=1, device_id=(lax.rem(chip + d, chips) * 2 + c, me_p), device_id_type=MESH)
    pl.semaphore_signal(barrier, inc=1, device_id=(partner, me_p), device_id_type=MESH)
    for d in range(1, n_p):
        pl.semaphore_signal(barrier, inc=1, device_id=(me_e, lax.rem(me_p + d, n_p)), device_id_type=MESH)
    pl.semaphore_wait(barrier, 2 * (chips - 1) + n_p)

    sends = []

    def go(copy):
        copy.start()
        sends.append(copy)
        return copy

    hub = chips == 4
    if hub:
        side = chip // 2
        end, inner = 3 * side, 1 + side
        far_end, far_inner = 3 - end, 3 - inner
        is_inner = chip == inner
        mate = jnp.where(is_inner, end, inner)
        targets = [far_inner, mate]
    else:
        targets = [lax.rem(chip + d, chips) for d in range(1, chips)]

    def send_to(j, i, to):
        mine, theirs = fb[j].at[chip, core], bo[j]
        return (remote(mine, mine, ag_send.at[j, i, 0], ag_recv.at[j, chip, core], to * 2 + core, me_p),
                remote(theirs, mine, ag_send.at[j, i, 1], ag_recv.at[j, chip, core], to * 2 + across, me_p))

    def send_own(j):
        for i, to in enumerate(targets):
            for copy in send_to(j, i, to):
                go(copy)
        go(remote(bo[j], fb[j].at[chip, core], ag_send.at[j, chips - 1, 1], ag_recv.at[j, chip, core], partner, me_p))

    def arrived(j, k, c):
        block = fb[j].at[k, c]
        remote(block, block, ag_send.at[j, 0, 0], ag_recv.at[j, k, c], partner, me_p).wait_recv()

    def pass_copy(j, i):
        k = (far_inner, far_end)[i]
        return remote(fb[j].at[k], fb[j].at[k], fw_send.at[j, i], ag_recv.at[j, k, 0], end * 2 + core, me_p)

    def pass_on(j):
        if not hub:
            return

        @pl.when(is_inner)
        def _():
            for i in range(2):
                k = (far_inner, far_end)[i]
                arrived(j, k, 0)
                arrived(j, k, 1)
                pass_copy(j, i).start()

    def complete(j):
        arrived(j, chip, across)
        if not hub:
            for to in targets:
                arrived(j, to, 0)
                arrived(j, to, 1)
            return
        arrived(j, mate, 0)
        arrived(j, mate, 1)

        @pl.when(jnp.logical_not(is_inner))
        def _():
            for i in range(2):
                pass_copy(j, i).wait_recv()

    for j in range(pieces):
        own[j].wait()
        far[j].wait()
        send_own(j)
        if j == 0:
            own[pieces].wait()
            tangents = [
                go(remote(tg.at[core, me_p], tg.at[core, me_p], tg_send.at[d], tg_recv.at[d],
                          me_e, lax.rem(me_p + d, n_p)))
                for d in range(1, n_p)
            ]
    theirs = lanes(across, 0, half)
    exchanged = [
        go(remote(src, dst, ex_send.at[i], ex_recv.at[i], partner, me_p))
        for i, (src, dst) in enumerate((
            (mask_h, mask.at[core]), (coef_h, coef.at[core]),
            (trans_h.at[:, theirs], trans.at[core]), (ivar_h.at[:, theirs], ivar.at[core])))
    ]
    block = TILE
    tiles = half // TILE
    used_rows[...] = jnp.zeros_like(used_rows)

    def weigh_all(c):
        used = mask[c].astype(jnp.float32)
        used_rows[c, :tiles, :] = jnp.where(core == 0, used[:tiles], used[tiles:])
        used_cols[c] = used_rows[c].T

        def weigh(r, _):
            at = pl.ds(pl.multiple_of(r * block, block), block)
            used = used_cols[c, at, :]
            for t in range(tiles):
                here = pl.ds(t * TILE, TILE)
                tr = trans[c, at, here].astype(jnp.float32)
                weights[c, at, here] = (
                    tr * tr * ivar[c, at, here].astype(jnp.float32)
                    * jnp.broadcast_to(used[:, t:t + 1], (block, TILE)))
            return 0

        lax.fori_loop(0, rows // block, weigh, 0)
        coef_t[c] = coef[c].T

    def first(c):
        tang[c] = tg[c].reshape(rank, rows).T

        def first_term(r, _):
            at = pl.ds(pl.multiple_of(r * block, block), block)
            for j in range(pieces):
                here = pl.ds(starts[j], widths[j])
                moved[c, at, here] = jnp.dot(tang[c, at, :], basis[:, here], preferred_element_type=jnp.float32)
            return 0

        lax.fori_loop(0, rows // block, first_term, 0)

    for copy in loads:
        copy.wait()
    weigh_all(core)
    pass_on(0)
    for copy in tangents:
        copy.wait_recv()
    other_tangent = go(remote(tg.at[core], tg.at[core], ex_send.at[4], ex_recv.at[4], partner, me_p))
    first(core)
    for j in range(1, pieces):
        pass_on(j)
    for copy in exchanged:
        copy.wait_recv()
    weigh_all(across)
    other_tangent.wait_recv()
    first(across)

    def other(i, me):
        return i + (i >= me).astype(jnp.int32)

    def slot_at(to, me):
        return jnp.where(me > to, me - 1, me)

    def swap_copy(to):
        return remote(cpart.at[across, to], cswap.at[to], sw_send.at[to], sw_recv.at[to], partner, me_p)

    def start_swap():
        for i in range(n_p - 1):
            swap_copy(other(i, me_p)).start()
        swap_copy(me_p).start()

    def work(j):
        width = widths[j]
        here = pl.ds(starts[j], width)
        last = j + 1 == pieces
        complete(j)
        if j:
            release(j - 1)
        full = fb[j][...].reshape(rank, width)

        def second(c):
            total = moved[c, :, here] + jnp.dot(coef[c], full, preferred_element_type=jnp.float32)
            wt[j][c] = (weights[c, :, here] * total).astype(jnp.bfloat16)

        def coef_part(c):
            cterm = lax.dot_general(
                basis[:, here], wt[j][c], (((1,), (1,)), ((), ())), preferred_element_type=jnp.float32
            ).reshape(n_p, cb, rows)
            cpart[c] = cterm if j == 0 else cpart[c] + cterm

        if last:
            second(across)
            coef_part(across)
            start_swap()
            second(core)
        else:
            second(0)
            second(1)
        term = (jnp.dot(coef_t[0], wt[j][0], preferred_element_type=jnp.float32)
                + jnp.dot(coef_t[1], wt[j][1], preferred_element_type=jnp.float32))
        part[j][...] = term.reshape(chips, 2, rank // n_e, width)
        scatter(j)
        own_rows(j)
        if not last:
            coef_part(0)
        coef_part(1 if not last else core)

    def rs_joint(j, i, to, slot):
        return (remote(rs_out[j].at[i], rs_in[j].at[slot], rs_send.at[j, i, 0], rs_recv.at[j, slot, 0],
                       to * 2 + core, me_p),
                remote(rs_fac_out[j].at[i], rs_fac_in[j].at[slot], rsf_send.at[j, i, 0], rsf_recv.at[j, slot, 0],
                       to * 2 + core, me_p))

    def rs_copies(j, i, c, to, slot, at):
        return (remote(rs_out[j].at[i, c], rs_in[j].at[slot, at], rs_send.at[j, i, c], rs_recv.at[j, slot, at],
                       to * 2 + c, me_p),
                remote(rs_fac_out[j].at[i, c], rs_fac_in[j].at[slot, at], rsf_send.at[j, i, c], rsf_recv.at[j, slot, at],
                       to * 2 + c, me_p))

    merged = [j + 1 < pieces for j in range(pieces)]

    def put(j, i, c, total):
        value, factor = scaled(total)
        rs_out[j][i, c] = value
        rs_fac_out[j][i, c] = factor

    def ship(j, i):
        to = other(i, chip)
        slot = slot_at(to, chip)
        for c in range(2):
            put(j, i, c, part[j][to, c])
            if not merged[j]:
                for copy in rs_copies(j, i, c, to, slot, core):
                    go(copy)

    def release(j):
        for i in range(chips - 1):
            to = other(i, chip)
            for copy in rs_joint(j, i, to, slot_at(to, chip)):
                go(copy)

    def scatter(j):
        for i in range(chips - 1):
            ship(j, i)

    def own_rows(j):
        if not merged[j]:
            go(remote(part[j].at[chip, across], pin[j], pin_send.at[j], pin_recv.at[j], partner, me_p))

    def reduced(j):
        if not merged[j]:
            return
        totals = [part[j][chip, c] for c in range(2)]
        for i in range(chips - 1):
            for copy in rs_joint(j, i, chip, i):
                copy.wait_recv()
            for c in range(2):
                totals[c] = totals[c] + restored(rs_in[j][i, c], rs_fac_in[j][i, c])
        for c in range(2):
            part[j][chip, c] = totals[c]
        go(remote(part[j].at[chip, across], pin[j], pin_send.at[j], pin_recv.at[j], partner, me_p))

    def gathered(j):
        remote(pin[j], pin[j], pin_send.at[j], pin_recv.at[j], partner, me_p).wait_recv()
        totals = [jnp.where(core == h, part[j][chip, core], pin[j][...]) for h in range(2)]
        for i in range(0 if merged[j] else chips - 1):
            for h in range(2):
                for copy in rs_copies(j, i, 0, chip, i, h):
                    copy.wait_recv()
                totals[h] = totals[h] + restored(rs_in[j][i, h], rs_fac_in[j][i, h])
        for h in range(2):
            at = h * half + starts[j]
            bout[:, at:at + widths[j]] = totals[h] * (1.0 / math.sqrt(rows * n_e))

    for j in range(pieces):
        work(j)

    for i in range(n_p - 1):
        to = other(i, me_p)
        slot = slot_at(to, me_p)
        swap_copy(to).wait_recv()
        value, factor = scaled(cpart[core, to] + cswap[to])
        cs_out[i] = value
        cs_fac_out[i] = factor
        go(remote(cs_out.at[i], cs_in.at[slot], cs_send.at[i], cs_recv.at[slot], me_e, to))
        go(remote(cs_fac_out.at[i], cs_fac_in.at[slot], csf_send.at[i], csf_recv.at[slot], me_e, to))
    swap_copy(me_p).wait_recv()

    for j in range(pieces):
        reduced(j)
    for j in range(pieces):
        gathered(j)
    total = cpart[core, me_p] + cswap[me_p]
    for i in range(n_p - 1):
        remote(cs_out.at[i], cs_in.at[i], cs_send.at[i], cs_recv.at[i], partner, me_p).wait_recv()
        remote(cs_fac_out.at[i], cs_fac_in.at[i], csf_send.at[i], csf_recv.at[i], partner, me_p).wait_recv()
        total = total + restored(cs_in[i], cs_fac_in[i])
    cout[...] = total * (1.0 / math.sqrt(half * 2 * n_p))

    for copy in sends:
        copy.wait_send()
    for i in range(n_p):
        swap_copy(i).wait_send()
    if hub:
        @pl.when(is_inner)
        def _():
            for j in range(pieces):
                for i in range(2):
                    pass_copy(j, i).wait_send()


def drain(a, b, x, y, sem):
    c0 = pltpu.make_async_copy(a, x, sem.at[0])
    c1 = pltpu.make_async_copy(b, y, sem.at[1])
    c1.start()
    c0.start()
    c1.wait()
    c0.wait()


def body(n_e, n_p, *args):
    trans, ivar, mask, coef, basis, ctan, btan = args
    rows, cols = trans.shape
    rank = coef.shape[1]
    chips = n_e // 2
    rb, cb = rank // n_e, rank // n_p
    widths = split_columns(cols)
    pieces = len(widths)
    half = cols // 2
    padded = -(-(half // TILE) // TILE) * TILE
    f32, bf16 = jnp.float32, jnp.bfloat16
    dma = pltpu.SemaphoreType.DMA
    V = pltpu.VMEM

    def each(shape, dtype):
        return [V(tuple(w if v is None else v for v in shape), dtype) for w in widths]

    coef_sum, basis_sum = pl.pallas_call(
        functools.partial(kernel, n_e, n_p, widths),
        out_shape=(pltpu.VMEM((cb, rows), f32), pltpu.VMEM((rb, cols), f32)),
        in_specs=[pl.BlockSpec(memory_space=pl.ANY)] * 7,
        out_specs=(pl.BlockSpec(memory_space=pltpu.VMEM),) * 2,
        scratch_shapes=[
            V((2, rows, half), bf16), V((2, rows, half), bf16), V((2, *mask.shape[::-1]), jnp.int32),
            V((2, rows, rank), bf16), V((rank, half), bf16), V((2, n_p, cb, rows), bf16),
            *each((chips, 2, rb, None), bf16), *each((rb, None), bf16),
            V((2, padded, rows), f32), V((2, rows, padded), f32),
            V((2, rows, rank), bf16), V((2, rank, rows), bf16), V((2, rows, half), f32), V((2, rows, half), f32),
            *each((2, rows, None), bf16),
            *each((chips, 2, rb, None), f32), *each((rb, None), f32),
            *each((chips - 1, 2, rb, None), WIRE), *each((chips - 1, 2, rb, None), WIRE),
            *each((chips - 1, 2, 1, None), f32), *each((chips - 1, 2, 1, None), f32),
            V((2, n_p, cb, rows), f32), V((n_p, cb, rows), f32), V((n_p, cb, rows), WIRE), V((n_p, cb, rows), WIRE),
            V((n_p, 1, rows), f32), V((n_p, 1, rows), f32),
            dma((5,)), dma((pieces + 1,)), dma((pieces,)),
            dma((n_p,)), dma((n_p,)), dma((pieces, chips, 2)), dma((pieces, chips, 2)), dma((pieces, 2)),
            dma((5,)), dma((5,)),
            dma((pieces,)), dma((pieces,)), dma((pieces, chips, 2)), dma((pieces, chips, 2)),
            dma((pieces, chips, 2)), dma((pieces, chips, 2)),
            dma((n_p,)), dma((n_p,)), dma((n_p,)), dma((n_p,)), dma((n_p,)), dma((n_p,)),
        ],
        compiler_params=pltpu.CompilerParams(
            collective_id=0, has_side_effects=True, vmem_limit_bytes=56 * 1024 * 1024
        ),
    )(trans, ivar, mask.T, coef, basis, ctan.T, btan)
    coef_grad, basis_grad = pl.pallas_call(
        drain,
        out_shape=(jax.ShapeDtypeStruct((cb, rows), f32), jax.ShapeDtypeStruct((rb, cols), f32)),
        in_specs=[pl.BlockSpec(memory_space=pltpu.VMEM)] * 2,
        out_specs=(pl.BlockSpec(memory_space=pl.ANY),) * 2,
        scratch_shapes=[dma((2,))],
    )(*[pltpu.with_memory_space_constraint(v, pltpu.VMEM) for v in (coef_sum, basis_sum)])
    return coef_grad.T, basis_grad


def solution(mesh):
    placed = (
        P("exp", "pix"),
        P("exp", "pix"),
        P("exp", "pix"),
        P("exp", None),
        P(None, "pix"),
        P("exp", "pix"),
        P("exp", "pix"),
    )
    return jax.shard_map(
        functools.partial(body, mesh.shape["exp"], mesh.shape["pix"]),
        mesh=mesh,
        in_specs=placed,
        out_specs=(P("exp", "pix"), P("exp", "pix")),
        check_vma=False,
    )
```

```python
import functools
import math

import jax
import jax.numpy as jnp
from jax import lax
from jax.experimental import pallas as pl
from jax.experimental.pallas import tpu as pltpu
from jax.sharding import PartitionSpec as P

TILE = 128
WIRE = jnp.int16
TOP = 32767.0
TINY = 1e-30
MESH = pl.DeviceIdType.MESH

def split_columns(cols):
    tiles = cols // (2 * TILE)
    first = tiles // 3
    return [TILE * v for v in (first, tiles - first) if v]


def scaled(x):
    peak = jnp.maximum(jnp.max(jnp.abs(x), axis=0, keepdims=True), TINY)
    return jnp.round(x * (TOP / peak)).astype(jnp.int32).astype(WIRE), peak * (1.0 / TOP)


def restored(value, factor):
    return value.astype(jnp.int32).astype(jnp.float32) * factor


def kernel(n_e, n_p, widths, trans_h, ivar_h, mask_h, coef_h, basis_h, ctan_h, btan_h, cout, bout, *scratch):
    scratch = list(scratch)

    def take(n=None):
        if n is None:
            return scratch.pop(0)
        return [scratch.pop(0) for _ in range(n)]

    pieces = len(widths)
    trans, ivar, mask, coef, basis, tg = take(6)
    fb, bo = take(pieces), take(pieces)
    used_rows, used_cols, tang, coef_t, weights, moved = take(6)
    wt, part, pin, rs_out, rs_in, rs_fac_out, rs_fac_in = (take(pieces) for _ in range(7))
    cpart, cswap, cs_out, cs_in, cs_fac_out, cs_fac_in = take(6)
    load_sem, own_sem, far_sem = take(3)
    tg_send, tg_recv, ag_send, ag_recv, fw_send, ex_send, ex_recv = take(7)
    pin_send, pin_recv, rs_send, rs_recv, rsf_send, rsf_recv = take(6)
    sw_send, sw_recv, cs_send, cs_recv, csf_send, csf_recv = take(6)
    assert not scratch
    rows, half = trans.shape[1:]
    rank = coef.shape[2]
    starts = [sum(widths[:j]) for j in range(pieces)]
    chips = n_e // 2
    cb = rank // n_p
    me_e, me_p = lax.axis_index("exp"), lax.axis_index("pix")
    core, chip = lax.rem(me_e, 2), me_e // 2
    across = 1 - core
    partner = chip * 2 + across

    def lanes(c, start, width):
        return pl.ds(pl.multiple_of(c * half + start, TILE), width)

    def remote(src, dst, send, recv, e, p):
        return pltpu.make_async_remote_copy(
            src_ref=src, dst_ref=dst, send_sem=send, recv_sem=recv,
            device_id=(e, p), device_id_type=MESH,
        )

    own, far = [], []
    for j in range(pieces):
        own.append(pltpu.make_async_copy(
            btan_h.at[:, lanes(core, starts[j], widths[j])], fb[j].at[chip, core], own_sem.at[j]))
        far.append(pltpu.make_async_copy(
            btan_h.at[:, lanes(across, starts[j], widths[j])], bo[j], far_sem.at[j]))
    own.append(pltpu.make_async_copy(ctan_h, tg.at[core, me_p], own_sem.at[pieces]))
    for copy in own[:pieces] + far + own[pieces:]:
        copy.start()
    mine = lanes(core, 0, half)
    loads = [
        pltpu.make_async_copy(src, dst, load_sem.at[i])
        for i, (src, dst) in enumerate((
            (trans_h.at[:, mine], trans.at[core]), (ivar_h.at[:, mine], ivar.at[core]), (mask_h, mask.at[core]),
            (coef_h, coef.at[core]), (basis_h.at[:, mine], basis)))
    ]
    for copy in loads:
        copy.start()

    barrier = pltpu.get_barrier_semaphore()
    for d in range(1, chips):
        for c in range(2):
            pl.semaphore_signal(barrier, inc=1, device_id=(lax.rem(chip + d, chips) * 2 + c, me_p), device_id_type=MESH)
    pl.semaphore_signal(barrier, inc=1, device_id=(partner, me_p), device_id_type=MESH)
    for d in range(1, n_p):
        pl.semaphore_signal(barrier, inc=1, device_id=(me_e, lax.rem(me_p + d, n_p)), device_id_type=MESH)
    pl.semaphore_wait(barrier, 2 * (chips - 1) + n_p)

    sends = []

    def go(copy):
        copy.start()
        sends.append(copy)
        return copy

    hub = chips == 4
    if hub:
        side = chip // 2
        end, inner = 3 * side, 1 + side
        far_end, far_inner = 3 - end, 3 - inner
        is_inner = chip == inner
        mate = jnp.where(is_inner, end, inner)
        targets = [far_inner, mate]
    else:
        targets = [lax.rem(chip + d, chips) for d in range(1, chips)]

    def send_to(j, i, to):
        mine, theirs = fb[j].at[chip, core], bo[j]
        return (remote(mine, mine, ag_send.at[j, i, 0], ag_recv.at[j, chip, core], to * 2 + core, me_p),
                remote(theirs, mine, ag_send.at[j, i, 1], ag_recv.at[j, chip, core], to * 2 + across, me_p))

    def send_own(j):
        for i, to in enumerate(targets):
            for copy in send_to(j, i, to):
                go(copy)
        go(remote(bo[j], fb[j].at[chip, core], ag_send.at[j, chips - 1, 1], ag_recv.at[j, chip, core], partner, me_p))

    def arrived(j, k, c):
        block = fb[j].at[k, c]
        remote(block, block, ag_send.at[j, 0, 0], ag_recv.at[j, k, c], partner, me_p).wait_recv()

    def pass_copy(j, i):
        k = (far_inner, far_end)[i]
        return remote(fb[j].at[k], fb[j].at[k], fw_send.at[j, i], ag_recv.at[j, k, 0], end * 2 + core, me_p)

    def pass_on(j):
        if not hub:
            return

        @pl.when(is_inner)
        def _():
            for i in range(2):
                k = (far_inner, far_end)[i]
                arrived(j, k, 0)
                arrived(j, k, 1)
                pass_copy(j, i).start()

    def complete(j):
        arrived(j, chip, across)
        if not hub:
            for to in targets:
                arrived(j, to, 0)
                arrived(j, to, 1)
            return
        arrived(j, mate, 0)
        arrived(j, mate, 1)

        @pl.when(jnp.logical_not(is_inner))
        def _():
            for i in range(2):
                pass_copy(j, i).wait_recv()

    for j in range(pieces):
        own[j].wait()
        far[j].wait()
        send_own(j)
        if j == 0:
            own[pieces].wait()
            tangents = [
                go(remote(tg.at[core, me_p], tg.at[core, me_p], tg_send.at[d], tg_recv.at[d],
                          me_e, lax.rem(me_p + d, n_p)))
                for d in range(1, n_p)
            ]
    theirs = lanes(across, 0, half)
    exchanged = [
        go(remote(src, dst, ex_send.at[i], ex_recv.at[i], partner, me_p))
        for i, (src, dst) in enumerate((
            (mask_h, mask.at[core]), (coef_h, coef.at[core]),
            (trans_h.at[:, theirs], trans.at[core]), (ivar_h.at[:, theirs], ivar.at[core])))
    ]
    block = TILE
    tiles = half // TILE
    used_rows[...] = jnp.zeros_like(used_rows)

    def weigh_all(c):
        used = mask[c].astype(jnp.float32)
        used_rows[c, :tiles, :] = jnp.where(core == 0, used[:tiles], used[tiles:])
        used_cols[c] = used_rows[c].T

        def weigh(r, _):
            at = pl.ds(pl.multiple_of(r * block, block), block)
            used = used_cols[c, at, :]
            for t in range(tiles):
                here = pl.ds(t * TILE, TILE)
                tr = trans[c, at, here].astype(jnp.float32)
                weights[c, at, here] = (
                    tr * tr * ivar[c, at, here].astype(jnp.float32)
                    * jnp.broadcast_to(used[:, t:t + 1], (block, TILE)))
            return 0

        lax.fori_loop(0, rows // block, weigh, 0)

    def first(c):
        tang[c] = tg[c].reshape(rank, rows).T

        def first_term(r, _):
            at = pl.ds(pl.multiple_of(r * block, block), block)
            for j in range(pieces):
                here = pl.ds(starts[j], widths[j])
                moved[c, at, here] = jnp.dot(tang[c, at, :], basis[:, here], preferred_element_type=jnp.float32)
            return 0

        lax.fori_loop(0, rows // block, first_term, 0)

    for copy in loads:
        copy.wait()
    weigh_all(core)
    pass_on(0)
    for copy in tangents:
        copy.wait_recv()
    other_tangent = go(remote(tg.at[core], tg.at[core], ex_send.at[4], ex_recv.at[4], partner, me_p))
    first(core)
    for j in range(1, pieces):
        pass_on(j)
    for copy in exchanged:
        copy.wait_recv()
    weigh_all(across)
    other_tangent.wait_recv()
    first(across)
    for c in range(2):
        coef_t[c] = coef[c].T

    def other(i, me):
        return i + (i >= me).astype(jnp.int32)

    def slot_at(to, me):
        return jnp.where(me > to, me - 1, me)

    def swap_copy(to):
        return remote(cpart.at[across, to], cswap.at[to], sw_send.at[to], sw_recv.at[to], partner, me_p)

    def start_swap():
        for i in range(n_p - 1):
            swap_copy(other(i, me_p)).start()
        swap_copy(me_p).start()

    def work(j):
        width = widths[j]
        here = pl.ds(starts[j], width)
        last = j + 1 == pieces
        complete(j)
        if j:
            release(j - 1)
        full = fb[j][...].reshape(rank, width)

        def second(c):
            total = moved[c, :, here] + jnp.dot(coef[c], full, preferred_element_type=jnp.float32)
            wt[j][c] = (weights[c, :, here] * total).astype(jnp.bfloat16)

        def coef_part(c):
            cterm = lax.dot_general(
                basis[:, here], wt[j][c], (((1,), (1,)), ((), ())), preferred_element_type=jnp.float32
            ).reshape(n_p, cb, rows)
            cpart[c] = cterm if j == 0 else cpart[c] + cterm

        if last:
            second(across)
            coef_part(across)
            start_swap()
            second(core)
        else:
            second(0)
            second(1)
        term = (jnp.dot(coef_t[0], wt[j][0], preferred_element_type=jnp.float32)
                + jnp.dot(coef_t[1], wt[j][1], preferred_element_type=jnp.float32))
        part[j][...] = term.reshape(chips, 2, rank // n_e, width)
        scatter(j)
        own_rows(j)
        if not last:
            coef_part(0)
        coef_part(1 if not last else core)

    def rs_joint(j, i, to, slot):
        return (remote(rs_out[j].at[i], rs_in[j].at[slot], rs_send.at[j, i, 0], rs_recv.at[j, slot, 0],
                       to * 2 + core, me_p),
                remote(rs_fac_out[j].at[i], rs_fac_in[j].at[slot], rsf_send.at[j, i, 0], rsf_recv.at[j, slot, 0],
                       to * 2 + core, me_p))

    def rs_copies(j, i, c, to, slot, at):
        return (remote(rs_out[j].at[i, c], rs_in[j].at[slot, at], rs_send.at[j, i, c], rs_recv.at[j, slot, at],
                       to * 2 + c, me_p),
                remote(rs_fac_out[j].at[i, c], rs_fac_in[j].at[slot, at], rsf_send.at[j, i, c], rsf_recv.at[j, slot, at],
                       to * 2 + c, me_p))

    merged = [j + 1 < pieces for j in range(pieces)]

    def put(j, i, c, total):
        value, factor = scaled(total)
        rs_out[j][i, c] = value
        rs_fac_out[j][i, c] = factor

    def ship(j, i):
        to = other(i, chip)
        slot = slot_at(to, chip)
        for c in range(2):
            put(j, i, c, part[j][to, c])
            if not merged[j]:
                for copy in rs_copies(j, i, c, to, slot, core):
                    go(copy)

    def release(j):
        for i in range(chips - 1):
            to = other(i, chip)
            for copy in rs_joint(j, i, to, slot_at(to, chip)):
                go(copy)

    def scatter(j):
        for i in range(chips - 1):
            ship(j, i)

    def own_rows(j):
        if not merged[j]:
            go(remote(part[j].at[chip, across], pin[j], pin_send.at[j], pin_recv.at[j], partner, me_p))

    def reduced(j):
        if not merged[j]:
            return
        totals = [part[j][chip, c] for c in range(2)]
        for i in range(chips - 1):
            for copy in rs_joint(j, i, chip, i):
                copy.wait_recv()
            for c in range(2):
                totals[c] = totals[c] + restored(rs_in[j][i, c], rs_fac_in[j][i, c])
        for c in range(2):
            part[j][chip, c] = totals[c]
        go(remote(part[j].at[chip, across], pin[j], pin_send.at[j], pin_recv.at[j], partner, me_p))

    def gathered(j):
        remote(pin[j], pin[j], pin_send.at[j], pin_recv.at[j], partner, me_p).wait_recv()
        totals = [jnp.where(core == h, part[j][chip, core], pin[j][...]) for h in range(2)]
        for i in range(0 if merged[j] else chips - 1):
            for h in range(2):
                for copy in rs_copies(j, i, 0, chip, i, h):
                    copy.wait_recv()
                totals[h] = totals[h] + restored(rs_in[j][i, h], rs_fac_in[j][i, h])
        for h in range(2):
            at = h * half + starts[j]
            bout[:, at:at + widths[j]] = totals[h] * (1.0 / math.sqrt(rows * n_e))

    for j in range(pieces):
        work(j)

    for i in range(n_p - 1):
        to = other(i, me_p)
        slot = slot_at(to, me_p)
        swap_copy(to).wait_recv()
        value, factor = scaled(cpart[core, to] + cswap[to])
        cs_out[i] = value
        cs_fac_out[i] = factor
        go(remote(cs_out.at[i], cs_in.at[slot], cs_send.at[i], cs_recv.at[slot], me_e, to))
        go(remote(cs_fac_out.at[i], cs_fac_in.at[slot], csf_send.at[i], csf_recv.at[slot], me_e, to))
    swap_copy(me_p).wait_recv()

    for j in range(pieces):
        reduced(j)
    for j in range(pieces):
        gathered(j)
    total = cpart[core, me_p] + cswap[me_p]
    for i in range(n_p - 1):
        remote(cs_out.at[i], cs_in.at[i], cs_send.at[i], cs_recv.at[i], partner, me_p).wait_recv()
        remote(cs_fac_out.at[i], cs_fac_in.at[i], csf_send.at[i], csf_recv.at[i], partner, me_p).wait_recv()
        total = total + restored(cs_in[i], cs_fac_in[i])
    cout[...] = total * (1.0 / math.sqrt(half * 2 * n_p))

    for copy in sends:
        copy.wait_send()
    for i in range(n_p):
        swap_copy(i).wait_send()
    if hub:
        @pl.when(is_inner)
        def _():
            for j in range(pieces):
                for i in range(2):
                    pass_copy(j, i).wait_send()


def drain(a, b, x, y, sem):
    c0 = pltpu.make_async_copy(a, x, sem.at[0])
    c1 = pltpu.make_async_copy(b, y, sem.at[1])
    c1.start()
    c0.start()
    c1.wait()
    c0.wait()


def body(n_e, n_p, *args):
    trans, ivar, mask, coef, basis, ctan, btan = args
    rows, cols = trans.shape
    rank = coef.shape[1]
    chips = n_e // 2
    rb, cb = rank // n_e, rank // n_p
    widths = split_columns(cols)
    pieces = len(widths)
    half = cols // 2
    padded = -(-(half // TILE) // TILE) * TILE
    f32, bf16 = jnp.float32, jnp.bfloat16
    dma = pltpu.SemaphoreType.DMA
    V = pltpu.VMEM

    def each(shape, dtype):
        return [V(tuple(w if v is None else v for v in shape), dtype) for w in widths]

    coef_sum, basis_sum = pl.pallas_call(
        functools.partial(kernel, n_e, n_p, widths),
        out_shape=(pltpu.VMEM((cb, rows), f32), pltpu.VMEM((rb, cols), f32)),
        in_specs=[pl.BlockSpec(memory_space=pl.ANY)] * 7,
        out_specs=(pl.BlockSpec(memory_space=pltpu.VMEM),) * 2,
        scratch_shapes=[
            V((2, rows, half), bf16), V((2, rows, half), bf16), V((2, *mask.shape[::-1]), jnp.int32),
            V((2, rows, rank), bf16), V((rank, half), bf16), V((2, n_p, cb, rows), bf16),
            *each((chips, 2, rb, None), bf16), *each((rb, None), bf16),
            V((2, padded, rows), f32), V((2, rows, padded), f32),
            V((2, rows, rank), bf16), V((2, rank, rows), bf16), V((2, rows, half), f32), V((2, rows, half), f32),
            *each((2, rows, None), bf16),
            *each((chips, 2, rb, None), f32), *each((rb, None), f32),
            *each((chips - 1, 2, rb, None), WIRE), *each((chips - 1, 2, rb, None), WIRE),
            *each((chips - 1, 2, 1, None), f32), *each((chips - 1, 2, 1, None), f32),
            V((2, n_p, cb, rows), f32), V((n_p, cb, rows), f32), V((n_p, cb, rows), WIRE), V((n_p, cb, rows), WIRE),
            V((n_p, 1, rows), f32), V((n_p, 1, rows), f32),
            dma((5,)), dma((pieces + 1,)), dma((pieces,)),
            dma((n_p,)), dma((n_p,)), dma((pieces, chips, 2)), dma((pieces, chips, 2)), dma((pieces, 2)),
            dma((5,)), dma((5,)),
            dma((pieces,)), dma((pieces,)), dma((pieces, chips, 2)), dma((pieces, chips, 2)),
            dma((pieces, chips, 2)), dma((pieces, chips, 2)),
            dma((n_p,)), dma((n_p,)), dma((n_p,)), dma((n_p,)), dma((n_p,)), dma((n_p,)),
        ],
        compiler_params=pltpu.CompilerParams(
            collective_id=0, has_side_effects=True, vmem_limit_bytes=56 * 1024 * 1024
        ),
    )(trans, ivar, mask.T, coef, basis, ctan.T, btan)
    coef_grad, basis_grad = pl.pallas_call(
        drain,
        out_shape=(jax.ShapeDtypeStruct((cb, rows), f32), jax.ShapeDtypeStruct((rb, cols), f32)),
        in_specs=[pl.BlockSpec(memory_space=pltpu.VMEM)] * 2,
        out_specs=(pl.BlockSpec(memory_space=pl.ANY),) * 2,
        scratch_shapes=[dma((2,))],
    )(*[pltpu.with_memory_space_constraint(v, pltpu.VMEM) for v in (coef_sum, basis_sum)])
    return coef_grad.T, basis_grad


def solution(mesh):
    placed = (
        P("exp", "pix"),
        P("exp", "pix"),
        P("exp", "pix"),
        P("exp", None),
        P(None, "pix"),
        P("exp", "pix"),
        P("exp", "pix"),
    )
    return jax.shard_map(
        functools.partial(body, mesh.shape["exp"], mesh.shape["pix"]),
        mesh=mesh,
        in_specs=placed,
        out_specs=(P("exp", "pix"), P("exp", "pix")),
        check_vma=False,
    )
```
